32 devices in a mesh: py: 4 (over z), px: 4 (over y, x), shift: 2 (over core).
Axes of the slice: x: 2, y: 2, z: 4, core: 2. Of those that a mesh axis runs over, the one named last changes fastest.
Arguments:
- right_side: float32 [512, 256, 256], P(('shift', 'py'), 'px'), parts along dimension 0, may hold values from -6 to 6
- first_guess: float32 [512, 256, 256], P(('shift', 'py'), 'px'), parts along dimension 0, may hold values from -6 to 6
- mass_term: float32 [512, 256, 256], P(('shift', 'py'), 'px'), parts along dimension 0, may hold values from 0.1 to 0.9
Outputs:
- corrected: float32 [512, 256, 256], P(('shift', 'py'), 'px'), parts along dimension 0
- remaining: float32 [512, 256, 256], P(('shift', 'py'), 'px'), parts along dimension 0
The draws below stay inside these ranges and needn't reach their ends.
There are 2 independent parts, one for each index of `shift`. The reference program is written for one: setup_inputs(seed, part) draws one part's arguments, and reference() takes and returns one part's arrays. A program takes and returns all parts, laid end to end along the dimension named above; each array names one. Nothing has to cross between parts.
All inputs are finite; a program needn't handle non-finite values.
Results may differ from the reference program's by a relative error of at most 0.000031.
Values sent between devices are 32-bit elements.
A program may use at most 128 MiB of HBM per device.

```python
import jax
import jax.numpy as jnp
from jax import lax

MEMBERS = 256
RATIO = 4
BEFORE = 2
AFTER = 3
INNER = 9
GRID_Y = 256
GRID_X = 256


def block_levels(key, shape, shards, low, largest):
    def one(axis_at, blocks):
        heights = jax.random.uniform(jax.random.fold_in(jax.random.fold_in(key, 6), axis_at), (blocks,), jnp.float32, low / len(shards), largest / len(shards))
        return jnp.repeat(jnp.exp(heights), shape[axis_at] // blocks).reshape((-1,) + (1,) * (len(shape) - axis_at - 1))

    gain = one(*shards[0])
    for cut in shards[1:]:
        gain = gain * one(*cut)
    return gain


def bell_draw(stream_key, shape, width, bound, shards=(), dtype=jnp.bfloat16):
    array = jax.random.normal(stream_key, shape, jnp.float32) * width
    if len(shards) > 0:
        array = block_levels(stream_key, shape, shards, -0.22, 0.18) * array
    return jnp.clip(array, min=-bound, max=bound).astype(dtype)


def setup_inputs(seed: int = 0, part: int = 0) -> dict:
    seeds = jax.random.split(jax.random.key(seed), 4)
    part_splits = jax.random.split(jax.random.fold_in(seeds[3], part), 4)
    return {
        "right_side": bell_draw(part_splits[0], (GRID_Y, GRID_X, MEMBERS), 1.0, 6.0, ((0, 4), (1, 4)), jnp.float32),
        "first_guess": bell_draw(part_splits[1], (GRID_Y, GRID_X, MEMBERS), 1.0, 6.0, ((0, 4), (1, 4)), jnp.float32),
        "mass_term": jnp.clip(0.1 + 0.79999997 * jax.random.uniform(part_splits[2], (GRID_Y, GRID_X, MEMBERS), jnp.float32) ** block_levels(part_splits[2], (GRID_Y, GRID_X, MEMBERS), ((0, 4), (1, 4)), -0.2, 0.2), 0.1, 0.9),
    }


def neighbour_sum(padded):
    inner_y, inner_x = padded.shape[0] - 2, padded.shape[1] - 2
    middle_rows = lax.slice_in_dim(padded, 1, 1 + inner_y, axis=0)
    middle_columns = lax.slice_in_dim(padded, 1, 1 + inner_x, axis=1)
    return (lax.slice_in_dim(middle_columns, 0, inner_y, axis=0) + lax.slice_in_dim(middle_columns, 2, 2 + inner_y, axis=0)
            + lax.slice_in_dim(middle_rows, 0, inner_x, axis=1) + lax.slice_in_dim(middle_rows, 2, 2 + inner_x, axis=1))


def sweep_once(padded, values, load, mass_here):
    return values + 0.8 * (load + neighbour_sum(padded) - (4.0 + mass_here) * values) / (4.0 + mass_here)


def block_means(values):
    cut = values.reshape(values.shape[0] // RATIO, RATIO, values.shape[1] // RATIO, RATIO, values.shape[2])
    return jnp.mean(cut, axis=(1, 3))


def spread_blocks(values):
    return jnp.repeat(jnp.repeat(values, RATIO, axis=0), RATIO, axis=1)


def reference(right_side, first_guess, mass_term):
    values = first_guess
    for sweep in range(BEFORE):
        values = sweep_once(jnp.pad(values, ((1, 1), (1, 1), (0, 0)), mode="wrap"), values, right_side, mass_term)
    defect = right_side + neighbour_sum(jnp.pad(values, ((1, 1), (1, 1), (0, 0)), mode="wrap")) - (4.0 + mass_term) * values
    coarse_load, coarse_mass = block_means(defect) * RATIO, block_means(mass_term) * RATIO
    coarse_values = jnp.zeros_like(coarse_load)
    for sweep in range(INNER):
        coarse_values = sweep_once(jnp.pad(coarse_values, ((1, 1), (1, 1), (0, 0)), mode="wrap"), coarse_values, coarse_load, coarse_mass)
    values = values + spread_blocks(coarse_values)
    for sweep in range(AFTER):
        values = sweep_once(jnp.pad(values, ((1, 1), (1, 1), (0, 0)), mode="wrap"), values, right_side, mass_term)
    corrected = values
    remaining = right_side + neighbour_sum(jnp.pad(corrected, ((1, 1), (1, 1), (0, 0)), mode="wrap")) - (4.0 + mass_term) * corrected
    return corrected, remaining
```

```python
import functools

import jax
import jax.numpy as jnp
from jax import lax
from jax.experimental import pallas as pl
from jax.experimental.pallas import tpu as pltpu
from jax.sharding import PartitionSpec as P

RATIO = 4
BEFORE = 2
AFTER = 3
INNER = 9
DAMP = 0.8
LANES = 128
PAD = 8


def kernel(
    sizes, counts, rhs_hbm, guess_hbm, mass_hbm, out_hbm, rem_hbm,
    u3, rhs3, d3, w2, rem3, tmp, cu2, cr2, cw2, hb,
    recv, send, crecv, csend, in_sem, out_sem, send_sem, recv_sem, csend_sem, crecv_sem,
):
    ny, nx, halves = sizes
    cy, cx = ny // RATIO, nx // RATIO
    pitch, cpitch = nx + 2 * PAD, cx + 2 * PAD
    n_py, n_px = counts
    py, px = lax.axis_index("py"), lax.axis_index("px")
    targets = (
        {"py": lax.rem(py + 1, n_py)},
        {"py": lax.rem(py + n_py - 1, n_py)},
        {"px": lax.rem(px + 1, n_px)},
        {"px": lax.rem(px + n_px - 1, n_px)},
    )
    u = u3.reshape(halves * 2 * (ny + 2) * pitch, LANES)
    rhs = rhs3.reshape(halves * ny * nx, LANES)
    d = d3.reshape(halves * ny * nx, LANES)
    rem = rem3.reshape(halves * ny * nx, LANES)

    loads = []
    for h in range(halves):
        lanes = pl.ds(h * LANES, LANES)
        loads.append((
            pltpu.make_async_copy(
                guess_hbm.at[:, :, lanes],
                u3.at[h, 0, pl.ds(1, ny), pl.ds(PAD, nx), :], in_sem.at[h, 0]),
            pltpu.make_async_copy(mass_hbm.at[:, :, lanes], d3.at[h], in_sem.at[h, 1]),
            pltpu.make_async_copy(rhs_hbm.at[:, :, lanes], rhs3.at[h], in_sem.at[h, 2]),
        ))
    for k in range(3):
        for h in range(halves):
            loads[h][k].start()

    barrier = pltpu.get_barrier_semaphore()
    for target in targets:
        pl.semaphore_signal(barrier, inc=1, device_id=target, device_id_type=pl.DeviceIdType.MESH)

    def ub(h, pp, y):
        return pl.multiple_of(((h * 2 + pp) * (ny + 2) + y + 1) * pitch + PAD, 8)

    def fb(h, y):
        return pl.multiple_of((h * ny + y) * nx, 8)

    def cub(h, pp, y):
        return pl.multiple_of(((h * 2 + pp) * (cy + 2) + y + 1) * cpitch + PAD, 8)

    def cfb(h, y):
        return pl.multiple_of((h * cy + y) * cx, 8)

    side = jnp.zeros((PAD, LANES), jnp.float32)
    for h in range(halves):
        for pp in range(2):
            for y in (-1, ny):
                u[pl.ds(ub(h, pp, y), nx), :] = jnp.zeros((nx, LANES), jnp.float32)
            for y in (-1, cy):
                cu2[pl.ds(cub(h, pp, y), cx), :] = jnp.zeros((cx, LANES), jnp.float32)

            def clear(y, _, h=h, pp=pp):
                u[pl.ds(ub(h, pp, y) - PAD, PAD), :] = side
                u[pl.ds(ub(h, pp, y) + nx, PAD), :] = side
                return 0

            lax.fori_loop(0, ny, clear, 0, unroll=4)

            def cclear(y, _, h=h, pp=pp):
                cu2[pl.ds(cub(h, pp, y) - PAD, PAD), :] = side
                cu2[pl.ds(cub(h, pp, y) + cx, PAD), :] = side
                return 0

            lax.fori_loop(0, cy, cclear, 0, unroll=4)

    pl.semaphore_wait(barrier, 4)

    def edges(array, base, step, h, pp, rows, columns):
        first = base(h, pp, 0)
        return (
            array[pl.ds(base(h, pp, rows - 1), columns), :],
            array[pl.ds(first, columns), :],
            array[pl.ds(first + columns - 1, rows, stride=step), :],
            array[pl.ds(first, rows, stride=step), :],
        )

    def copies(e, h, coarse):
        s, r, ss, rs = (csend, crecv, csend_sem, crecv_sem) if coarse else (send, recv, send_sem, recv_sem)
        return [
            pltpu.make_async_remote_copy(
                src_ref=s.at[e, h, k], dst_ref=r.at[e, h, k],
                send_sem=ss.at[e, h, k], recv_sem=rs.at[e, h, k],
                device_id=targets[k], device_id_type=pl.DeviceIdType.MESH)
            for k in range(4)
        ]

    started = []

    def exchange(e, h, pp, coarse=False):
        if coarse:
            cells = edges(cu2, cub, cpitch, h, pp, cy, cx)
        else:
            cells = edges(u, ub, pitch, h, pp, ny, nx)
        buffer = csend if coarse else send
        for k in range(4):
            buffer[e, h, k] = cells[k]
        out = copies(e, h, coarse)
        for k in (2, 3, 0, 1):
            out[k].start()
        started.append(out)

    def arrived(e, h, coarse=False):
        for copy in copies(e, h, coarse):
            copy.wait_recv()

    def around(b):
        return (u[pl.ds(b - pitch, nx), :] + u[pl.ds(b + pitch, nx), :]) + (
            u[pl.ds(b - 1, nx), :] + u[pl.ds(b + 1, nx), :])

    def sweep(h, pp):
        def body(y, _):
            b = ub(h, pp, y)
            f = pl.ds(fb(h, y), nx)
            u[pl.ds(ub(h, 1 - pp, y), nx), :] = (1.0 - DAMP) * u[pl.ds(b, nx), :] + w2[f, :] * (
                rhs[f, :] + around(b))
            return 0

        lax.fori_loop(0, ny, body, 0, unroll=2)

    def add_edges(array, base, step, weights, wbase, h, pp, rows, columns, values):
        first, wfirst = base(h, pp, 0), wbase(h, 0)
        places = (
            (pl.ds(first, columns), pl.ds(wfirst, columns)),
            (pl.ds(base(h, pp, rows - 1), columns), pl.ds(wbase(h, rows - 1), columns)),
            (pl.ds(first, rows, stride=step), pl.ds(wfirst, rows, stride=columns)),
            (pl.ds(first + columns - 1, rows, stride=step),
             pl.ds(wfirst + columns - 1, rows, stride=columns)),
        )
        for (place, wplace), value in zip(places, values):
            if weights is not None:
                value = weights[wplace, :] * value
            array[place, :] = array[place, :] + value

    def fold(array, start, size):
        total = array[pl.ds(start, size, stride=RATIO), :]
        for j in range(1, RATIO):
            total = total + array[pl.ds(start + j, size, stride=RATIO), :]
        return total * (1.0 / RATIO)

    def masses(h):
        def body(row, _):
            total = jnp.zeros((nx, LANES), jnp.float32)
            for j in range(RATIO):
                f = pl.ds(fb(h, row * RATIO + j), nx)
                m = d[f, :]
                total = total + m
                m = 4.0 + m
                d[f, :] = m
                w2[f, :] = DAMP / m
            t = pl.multiple_of(row * nx, 8)
            tmp[pl.ds(t, nx), :] = total
            cw2[pl.ds(cfb(h, row), cx), :] = DAMP / (4.0 + fold(tmp, t, cx))
            return 0

        lax.fori_loop(0, cy, body, 0)

    for h in range(halves):
        loads[h][0].wait()
        exchange(0, h, 0)
    for h in range(halves):
        loads[h][1].wait()
        masses(h)
        loads[h][2].wait()
        sweep(h, 0)
    pp = 0
    for e in range(BEFORE):
        pp = 1 - pp
        for h in range(halves):
            arrived(e, h)
            add_edges(u, ub, pitch, w2, fb, h, pp, ny, nx, [recv[e, h, k] for k in range(4)])
            exchange(e + 1, h, pp)
            if e + 1 < BEFORE:
                sweep(h, pp)

    def defect(h):
        def body(row, _):
            total = jnp.zeros((nx, LANES), jnp.float32)
            for j in range(RATIO):
                y = row * RATIO + j
                b = ub(h, pp, y)
                f = pl.ds(fb(h, y), nx)
                total = total + (rhs[f, :] + around(b) - d[f, :] * u[pl.ds(b, nx), :])
            t = pl.multiple_of(row * nx, 8)
            tmp[pl.ds(t, nx), :] = total
            cr2[pl.ds(cfb(h, row), cx), :] = fold(tmp, t, cx)
            return 0

        lax.fori_loop(0, cy, body, 0)

    for h in range(halves):
        defect(h)
    cpp = 0
    flat = recv.reshape((BEFORE + AFTER + 1) * halves * 4 * nx, LANES)
    for h in range(halves):
        arrived(BEFORE, h)
        values = [fold(flat, ((BEFORE * halves + h) * 4 + k) * nx, cx) for k in range(4)]
        add_edges(cr2, lambda h, pp, y: cfb(h, y), cx, None, cfb, h, 0, cy, cx, values)

        def start(row, _, h=h):
            f = pl.ds(cfb(h, row), cx)
            cu2[pl.ds(cub(h, 0, row), cx), :] = cw2[f, :] * cr2[f, :]
            return 0

        lax.fori_loop(0, cy, start, 0, unroll=4)
        exchange(0, h, 0, True)

    def csweep(h, pp):
        def body(y, _):
            b = cub(h, pp, y)
            f = pl.ds(cfb(h, y), cx)
            total = (cu2[pl.ds(b - cpitch, cx), :] + cu2[pl.ds(b + cpitch, cx), :]) + (
                cu2[pl.ds(b - 1, cx), :] + cu2[pl.ds(b + 1, cx), :])
            cu2[pl.ds(cub(h, 1 - pp, y), cx), :] = (1.0 - DAMP) * cu2[pl.ds(b, cx), :] + cw2[f, :] * (
                cr2[f, :] + total)
            return 0

        lax.fori_loop(0, cy, body, 0, unroll=4)

    for e in range(INNER - 1):
        for h in range(halves):
            csweep(h, cpp)
        cpp = 1 - cpp
        for h in range(halves):
            arrived(e, h, True)
            add_edges(cu2, cub, cpitch, cw2, cfb, h, cpp, cy, cx, [crecv[e, h, k] for k in range(4)])
            exchange(e + 1, h, cpp, True)

    for h in range(halves):
        def correct(row, _, h=h):
            t = pl.multiple_of(row * nx, 8)
            c = cu2[pl.ds(cub(h, cpp, row), cx), :]
            for j in range(RATIO):
                tmp[pl.ds(t + j, cx, stride=RATIO), :] = c
            c = tmp[pl.ds(t, nx), :]
            for j in range(RATIO):
                place = pl.ds(ub(h, pp, row * RATIO + j), nx)
                u[place, :] = u[place, :] + c
            return 0

        lax.fori_loop(0, cy, correct, 0)
        sweep(h, pp)
    pp = 1 - pp
    for h in range(halves):
        arrived(INNER - 1, h, True)
        values = []
        for k in range(4):
            c = crecv[INNER - 1, h, k]
            at = (h * 4 + k) * nx
            for j in range(RATIO):
                hb[pl.ds(at + j, cx, stride=RATIO), :] = c
            values.append(recv[BEFORE, h, k] + hb[pl.ds(at, nx), :])
        add_edges(u, ub, pitch, w2, fb, h, pp, ny, nx, values)
        exchange(BEFORE + 1, h, pp)
        sweep(h, pp)
    outs = []
    for e in range(BEFORE + 1, BEFORE + AFTER):
        pp = 1 - pp
        for h in range(halves):
            arrived(e, h)
            add_edges(u, ub, pitch, w2, fb, h, pp, ny, nx, [recv[e, h, k] for k in range(4)])
            exchange(e + 1, h, pp)
            if e + 1 < BEFORE + AFTER:
                sweep(h, pp)
            else:
                outs.append(pltpu.make_async_copy(
                    u3.at[h, pp, pl.ds(1, ny), pl.ds(PAD, nx), :],
                    out_hbm.at[:, :, pl.ds(h * LANES, LANES)], out_sem.at[h, 0]))
                outs[-1].start()

    for h in range(halves):
        def left(y, _, h=h):
            b = ub(h, pp, y)
            f = pl.ds(fb(h, y), nx)
            rem[f, :] = rhs[f, :] + around(b) - d[f, :] * u[pl.ds(b, nx), :]
            return 0

        lax.fori_loop(0, ny, left, 0, unroll=2)
    e = BEFORE + AFTER
    for h in range(halves):
        arrived(e, h)
        add_edges(rem, lambda h, pp, y: fb(h, y), nx, None, fb, h, 0, ny, nx,
                  [recv[e, h, k] for k in range(4)])
        outs.append(pltpu.make_async_copy(
            rem3.at[h], rem_hbm.at[:, :, pl.ds(h * LANES, LANES)], out_sem.at[h, 1]))
        outs[-1].start()
    for group in started:
        for copy in group:
            copy.wait_send()
    for copy in outs:
        copy.wait()


def shards(right_side, first_guess, mass_term):
    ny, nx, members = right_side.shape
    halves = members // LANES
    cy, cx = ny // RATIO, nx // RATIO
    fine, coarse = BEFORE + AFTER + 1, INNER
    vmem = lambda *shape: pltpu.VMEM(shape, jnp.float32)
    dma = lambda *shape: pltpu.SemaphoreType.DMA(shape)
    counts = (lax.axis_size("py"), lax.axis_size("px"))
    return pl.pallas_call(
        functools.partial(kernel, (ny, nx, halves), counts),
        out_shape=[jax.ShapeDtypeStruct(right_side.shape, jnp.float32)] * 2,
        in_specs=[pl.BlockSpec(memory_space=pl.ANY)] * 3,
        out_specs=[pl.BlockSpec(memory_space=pl.ANY)] * 2,
        scratch_shapes=[
            vmem(halves, 2, ny + 2, nx + 2 * PAD, LANES),
            vmem(halves, ny, nx, LANES),
            vmem(halves, ny, nx, LANES),
            vmem(halves * ny * nx, LANES),
            vmem(halves, ny, nx, LANES),
            vmem(cy * nx, LANES),
            vmem(halves * 2 * (cy + 2) * (cx + 2 * PAD), LANES),
            vmem(halves * cy * cx, LANES),
            vmem(halves * cy * cx, LANES),
            vmem(halves * 4 * nx, LANES),
            vmem(fine, halves, 4, nx, LANES),
            vmem(fine, halves, 4, nx, LANES),
            vmem(coarse, halves, 4, cx, LANES),
            vmem(coarse, halves, 4, cx, LANES),
            dma(halves, 3),
            dma(halves, 2),
            dma(fine, halves, 4),
            dma(fine, halves, 4),
            dma(coarse, halves, 4),
            dma(coarse, halves, 4),
        ],
        compiler_params=pltpu.CompilerParams(
            collective_id=0, has_side_effects=True, vmem_limit_bytes=50 * 1024 * 1024),
        name="two_grid",
    )(right_side, first_guess, mass_term)


def solution(mesh):
    spec = P(("shift", "py"), "px", None)
    return jax.shard_map(
        shards, mesh=mesh, in_specs=(spec,) * 3, out_specs=(spec,) * 2, check_vma=False)
```

```python
import functools

import jax
import jax.numpy as jnp
from jax import lax
from jax.experimental import pallas as pl
from jax.experimental.pallas import tpu as pltpu
from jax.sharding import PartitionSpec as P

RATIO = 4
BEFORE = 2
AFTER = 3
INNER = 9
DAMP = 0.8
LANES = 128
PAD = 8


def kernel(
    sizes, counts, rhs_hbm, guess_hbm, mass_hbm, out_hbm, rem_hbm,
    u3, rhs3, d3, w2, rem3, tmp, cu2, cr2, cw2, hb,
    recv, send, crecv, csend, in_sem, out_sem, send_sem, recv_sem, csend_sem, crecv_sem,
):
    ny, nx, halves = sizes
    cy, cx = ny // RATIO, nx // RATIO
    pitch, cpitch = nx + 2 * PAD, cx + 2 * PAD
    n_py, n_px = counts
    py, px = lax.axis_index("py"), lax.axis_index("px")
    targets = (
        {"py": lax.rem(py + 1, n_py)},
        {"py": lax.rem(py + n_py - 1, n_py)},
        {"px": lax.rem(px + 1, n_px)},
        {"px": lax.rem(px + n_px - 1, n_px)},
    )
    u = u3.reshape(halves * 2 * (ny + 2) * pitch, LANES)
    rhs = rhs3.reshape(halves * ny * nx, LANES)
    d = d3.reshape(halves * ny * nx, LANES)
    rem = rem3.reshape(halves * ny * nx, LANES)

    loads = []
    for h in range(halves):
        lanes = pl.ds(h * LANES, LANES)
        loads.append((
            pltpu.make_async_copy(
                guess_hbm.at[:, :, lanes],
                u3.at[h, 0, pl.ds(1, ny), pl.ds(PAD, nx), :], in_sem.at[h, 0]),
            pltpu.make_async_copy(mass_hbm.at[:, :, lanes], d3.at[h], in_sem.at[h, 1]),
            pltpu.make_async_copy(rhs_hbm.at[:, :, lanes], rhs3.at[h], in_sem.at[h, 2]),
        ))
    for k in range(3):
        for h in range(halves):
            loads[h][k].start()

    barrier = pltpu.get_barrier_semaphore()
    for target in targets:
        pl.semaphore_signal(barrier, inc=1, device_id=target, device_id_type=pl.DeviceIdType.MESH)

    def ub(h, pp, y):
        return pl.multiple_of(((h * 2 + pp) * (ny + 2) + y + 1) * pitch + PAD, 8)

    def fb(h, y):
        return pl.multiple_of((h * ny + y) * nx, 8)

    def cub(h, pp, y):
        return pl.multiple_of(((h * 2 + pp) * (cy + 2) + y + 1) * cpitch + PAD, 8)

    def cfb(h, y):
        return pl.multiple_of((h * cy + y) * cx, 8)

    side = jnp.zeros((PAD, LANES), jnp.float32)
    for h in range(halves):
        for pp in range(2):
            for y in (-1, ny):
                u[pl.ds(ub(h, pp, y), nx), :] = jnp.zeros((nx, LANES), jnp.float32)
            for y in (-1, cy):
                cu2[pl.ds(cub(h, pp, y), cx), :] = jnp.zeros((cx, LANES), jnp.float32)

            def clear(y, _, h=h, pp=pp):
                u[pl.ds(ub(h, pp, y) - PAD, PAD), :] = side
                u[pl.ds(ub(h, pp, y) + nx, PAD), :] = side
                return 0

            lax.fori_loop(0, ny, clear, 0, unroll=4)

            def cclear(y, _, h=h, pp=pp):
                cu2[pl.ds(cub(h, pp, y) - PAD, PAD), :] = side
                cu2[pl.ds(cub(h, pp, y) + cx, PAD), :] = side
                return 0

            lax.fori_loop(0, cy, cclear, 0, unroll=4)

    pl.semaphore_wait(barrier, 4)

    def edges(array, base, step, h, pp, rows, columns):
        first = base(h, pp, 0)
        return (
            array[pl.ds(base(h, pp, rows - 1), columns), :],
            array[pl.ds(first, columns), :],
            array[pl.ds(first + columns - 1, rows, stride=step), :],
            array[pl.ds(first, rows, stride=step), :],
        )

    def copies(e, h, coarse):
        s, r, ss, rs = (csend, crecv, csend_sem, crecv_sem) if coarse else (send, recv, send_sem, recv_sem)
        return [
            pltpu.make_async_remote_copy(
                src_ref=s.at[e, h, k], dst_ref=r.at[e, h, k],
                send_sem=ss.at[e, h, k], recv_sem=rs.at[e, h, k],
                device_id=targets[k], device_id_type=pl.DeviceIdType.MESH)
            for k in range(4)
        ]

    started = []

    def exchange(e, h, pp, coarse=False):
        if coarse:
            cells = edges(cu2, cub, cpitch, h, pp, cy, cx)
        else:
            cells = edges(u, ub, pitch, h, pp, ny, nx)
        buffer = csend if coarse else send
        for k in range(4):
            buffer[e, h, k] = cells[k]
        out = copies(e, h, coarse)
        for k in (2, 3, 0, 1):
            out[k].start()
        started.append(out)

    def arrived(e, h, coarse=False):
        for copy in copies(e, h, coarse):
            copy.wait_recv()

    def around(b):
        return (u[pl.ds(b - pitch, nx), :] + u[pl.ds(b + pitch, nx), :]) + (
            u[pl.ds(b - 1, nx), :] + u[pl.ds(b + 1, nx), :])

    def sweep(h, pp):
        def body(y, _):
            b = ub(h, pp, y)
            f = pl.ds(fb(h, y), nx)
            u[pl.ds(ub(h, 1 - pp, y), nx), :] = (1.0 - DAMP) * u[pl.ds(b, nx), :] + w2[f, :] * (
                rhs[f, :] + around(b))
            return 0

        lax.fori_loop(0, ny, body, 0, unroll=2)

    def add_edges(array, base, step, weights, wbase, h, pp, rows, columns, values):
        first, wfirst = base(h, pp, 0), wbase(h, 0)
        places = (
            (pl.ds(first, columns), pl.ds(wfirst, columns)),
            (pl.ds(base(h, pp, rows - 1), columns), pl.ds(wbase(h, rows - 1), columns)),
            (pl.ds(first, rows, stride=step), pl.ds(wfirst, rows, stride=columns)),
            (pl.ds(first + columns - 1, rows, stride=step),
             pl.ds(wfirst + columns - 1, rows, stride=columns)),
        )
        for (place, wplace), value in zip(places, values):
            if weights is not None:
                value = weights[wplace, :] * value
            array[place, :] = array[place, :] + value

    def fold(array, start, size):
        total = array[pl.ds(start, size, stride=RATIO), :]
        for j in range(1, RATIO):
            total = total + array[pl.ds(start + j, size, stride=RATIO), :]
        return total * (1.0 / RATIO)

    def masses(h):
        def body(row, _):
            total = jnp.zeros((nx, LANES), jnp.float32)
            for j in range(RATIO):
                f = pl.ds(fb(h, row * RATIO + j), nx)
                m = d[f, :]
                total = total + m
                m = 4.0 + m
                d[f, :] = m
                w2[f, :] = DAMP / m
            t = pl.multiple_of(row * nx, 8)
            tmp[pl.ds(t, nx), :] = total
            cw2[pl.ds(cfb(h, row), cx), :] = DAMP / (4.0 + fold(tmp, t, cx))
            return 0

        lax.fori_loop(0, cy, body, 0)

    for h in range(halves):
        loads[h][0].wait()
        exchange(0, h, 0)
    for h in range(halves):
        loads[h][1].wait()
        masses(h)
        loads[h][2].wait()
        sweep(h, 0)
    pp = 0
    for e in range(BEFORE):
        pp = 1 - pp
        for h in range(halves):
            arrived(e, h)
            add_edges(u, ub, pitch, w2, fb, h, pp, ny, nx, [recv[e, h, k] for k in range(4)])
            exchange(e + 1, h, pp)
            if e + 1 < BEFORE:
                sweep(h, pp)

    def defect(h):
        def body(row, _):
            total = jnp.zeros((nx, LANES), jnp.float32)
            for j in range(RATIO):
                y = row * RATIO + j
                b = ub(h, pp, y)
                f = pl.ds(fb(h, y), nx)
                total = total + (rhs[f, :] + around(b) - d[f, :] * u[pl.ds(b, nx), :])
            t = pl.multiple_of(row * nx, 8)
            tmp[pl.ds(t, nx), :] = total
            cr2[pl.ds(cfb(h, row), cx), :] = fold(tmp, t, cx)
            return 0

        lax.fori_loop(0, cy, body, 0)

    for h in range(halves):
        defect(h)
    cpp = 0
    flat = recv.reshape((BEFORE + AFTER + 1) * halves * 4 * nx, LANES)
    for h in range(halves):
        arrived(BEFORE, h)
        values = [fold(flat, ((BEFORE * halves + h) * 4 + k) * nx, cx) for k in range(4)]
        add_edges(cr2, lambda h, pp, y: cfb(h, y), cx, None, cfb, h, 0, cy, cx, values)

        def start(row, _, h=h):
            f = pl.ds(cfb(h, row), cx)
            cu2[pl.ds(cub(h, 0, row), cx), :] = cw2[f, :] * cr2[f, :]
            return 0

        lax.fori_loop(0, cy, start, 0, unroll=4)
        exchange(0, h, 0, True)

    def csweep(h, pp):
        def body(y, _):
            b = cub(h, pp, y)
            f = pl.ds(cfb(h, y), cx)
            total = (cu2[pl.ds(b - cpitch, cx), :] + cu2[pl.ds(b + cpitch, cx), :]) + (
                cu2[pl.ds(b - 1, cx), :] + cu2[pl.ds(b + 1, cx), :])
            cu2[pl.ds(cub(h, 1 - pp, y), cx), :] = (1.0 - DAMP) * cu2[pl.ds(b, cx), :] + cw2[f, :] * (
                cr2[f, :] + total)
            return 0

        lax.fori_loop(0, cy, body, 0, unroll=4)

    for e in range(INNER - 1):
        for h in range(halves):
            csweep(h, cpp)
        cpp = 1 - cpp
        for h in range(halves):
            arrived(e, h, True)
            add_edges(cu2, cub, cpitch, cw2, cfb, h, cpp, cy, cx, [crecv[e, h, k] for k in range(4)])
            exchange(e + 1, h, cpp, True)

    for h in range(halves):
        def correct(row, _, h=h):
            t = pl.multiple_of(row * nx, 8)
            c = cu2[pl.ds(cub(h, cpp, row), cx), :]
            for j in range(RATIO):
                tmp[pl.ds(t + j, cx, stride=RATIO), :] = c
            c = tmp[pl.ds(t, nx), :]
            for j in range(RATIO):
                place = pl.ds(ub(h, pp, row * RATIO + j), nx)
                u[place, :] = u[place, :] + c
            return 0

        lax.fori_loop(0, cy, correct, 0)
        sweep(h, pp)
    pp = 1 - pp
    for h in range(halves):
        arrived(INNER - 1, h, True)
        values = []
        for k in range(4):
            c = crecv[INNER - 1, h, k]
            at = (h * 4 + k) * nx
            for j in range(RATIO):
                hb[pl.ds(at + j, cx, stride=RATIO), :] = c
            values.append(recv[BEFORE, h, k] + hb[pl.ds(at, nx), :])
        add_edges(u, ub, pitch, w2, fb, h, pp, ny, nx, values)
        exchange(BEFORE + 1, h, pp)
        sweep(h, pp)
    outs = []
    for e in range(BEFORE + 1, BEFORE + AFTER):
        pp = 1 - pp
        for h in range(halves):
            arrived(e, h)
            add_edges(u, ub, pitch, w2, fb, h, pp, ny, nx, [recv[e, h, k] for k in range(4)])
            exchange(e + 1, h, pp)
            if e + 1 < BEFORE + AFTER:
                sweep(h, pp)
            else:
                outs.append(pltpu.make_async_copy(
                    u3.at[h, pp, pl.ds(1, ny), pl.ds(PAD, nx), :],
                    out_hbm.at[:, :, pl.ds(h * LANES, LANES)], out_sem.at[h, 0]))
                outs[-1].start()

    for h in range(halves):
        def left(y, _, h=h):
            b = ub(h, pp, y)
            f = pl.ds(fb(h, y), nx)
            rem[f, :] = rhs[f, :] + around(b) - d[f, :] * u[pl.ds(b, nx), :]
            return 0

        lax.fori_loop(0, ny, left, 0, unroll=2)
    e = BEFORE + AFTER
    for h in range(halves):
        arrived(e, h)
        add_edges(rem, lambda h, pp, y: fb(h, y), nx, None, fb, h, 0, ny, nx,
                  [recv[e, h, k] for k in range(4)])
        outs.append(pltpu.make_async_copy(
            rem3.at[h], rem_hbm.at[:, :, pl.ds(h * LANES, LANES)], out_sem.at[h, 1]))
        outs[-1].start()
    for group in started:
        for copy in group:
            copy.wait_send()
    for copy in outs:
        copy.wait()


def shards(right_side, first_guess, mass_term):
    ny, nx, members = right_side.shape
    halves = members // LANES
    cy, cx = ny // RATIO, nx // RATIO
    fine, coarse = BEFORE + AFTER + 1, INNER
    vmem = lambda *shape: pltpu.VMEM(shape, jnp.float32)
    dma = lambda *shape: pltpu.SemaphoreType.DMA(shape)
    counts = (lax.axis_size("py"), lax.axis_size("px"))
    return pl.pallas_call(
        functools.partial(kernel, (ny, nx, halves), counts),
        out_shape=[vmem(*right_side.shape)] * 2,
        in_specs=[pl.BlockSpec(memory_space=pl.ANY)] * 3,
        out_specs=[pl.BlockSpec(memory_space=pltpu.VMEM)] * 2,
        scratch_shapes=[
            vmem(halves, 2, ny + 2, nx + 2 * PAD, LANES),
            vmem(halves, ny, nx, LANES),
            vmem(halves, ny, nx, LANES),
            vmem(halves * ny * nx, LANES),
            vmem(halves, ny, nx, LANES),
            vmem(cy * nx, LANES),
            vmem(halves * 2 * (cy + 2) * (cx + 2 * PAD), LANES),
            vmem(halves * cy * cx, LANES),
            vmem(halves * cy * cx, LANES),
            vmem(halves * 4 * nx, LANES),
            vmem(fine, halves, 4, nx, LANES),
            vmem(fine, halves, 4, nx, LANES),
            vmem(coarse, halves, 4, cx, LANES),
            vmem(coarse, halves, 4, cx, LANES),
            dma(halves, 3),
            dma(halves, 2),
            dma(fine, halves, 4),
            dma(fine, halves, 4),
            dma(coarse, halves, 4),
            dma(coarse, halves, 4),
        ],
        compiler_params=pltpu.CompilerParams(
            collective_id=0, has_side_effects=True, vmem_limit_bytes=44 * 1024 * 1024),
        name="two_grid",
    )(right_side, first_guess, mass_term)


def solution(mesh):
    spec = P(("shift", "py"), "px", None)
    return jax.shard_map(
        shards, mesh=mesh, in_specs=(spec,) * 3, out_specs=(spec,) * 2, check_vma=False)
```
